128 devices in a mesh: tm: 8 (over x, core), batch: 16 (over z, y).
Axes of the slice: x: 4, y: 4, z: 4, core: 2. Of those that a mesh axis runs over, the one named last changes fastest.
Arguments:
- latents: float32 [8, 32, 4096], P('tm', None, 'batch'), may hold values from -6 to 6
- shifts: int32 [32], replicated, may hold values from 0 to 7
- starts: int32 [32], replicated, may hold values from 0 to 2
- labels: int32 [32], replicated, may hold values from 0 to 1000
- class_table: bfloat16 [1001, 1152], replicated, may hold values from -6 to 6
- w_freq: bfloat16 [256, 1152], replicated, may hold values from -0.375 to 0.375
- w_time: bfloat16 [1152, 1152], replicated, may hold values from -0.1875 to 0.1875
- w_ada: bfloat16 [1152, 9216], P(None, 'tm'), may hold values from -0.1875 to 0.1875
- w_patch: bfloat16 [16, 1152], replicated, may hold values from -1.5 to 1.5
- w_qkv: bfloat16 [1152, 3456], P('batch', 'tm'), may hold values from -1 to 1
- w_proj: bfloat16 [1152, 1152], P('tm', 'batch'), may hold values from -0.1875 to 0.1875
- w_fc1: bfloat16 [1152, 4608], P('batch', 'tm'), may hold values from -0.1875 to 0.1875
- w_fc2: bfloat16 [4608, 1152], P('tm', 'batch'), may hold values from -0.09375 to 0.09375
- w_final: bfloat16 [1152, 16], replicated, may hold values from -0.1875 to 0.1875
Outputs:
- new_latents: float32 [8, 32, 4096], P('tm', None, 'batch')
- velocity: bfloat16 [8, 32, 4096], P('tm', None, 'batch')
The draws below stay inside these ranges and needn't reach their ends.
All inputs are finite; a program needn't handle non-finite values.
Results may differ from the reference program's by a relative error of at most 0.0091.
Values may be sent and summed in bfloat16 or wider, within the bound.
A program may use at most 128 MiB of HBM per device.

```python
import math
import jax
import jax.numpy as jnp
from jax import lax

D = 1152
HEADS = 16
FF = 4608
FREQ = 256
NCLASS = 1001
GRID = 16
WIN = 8
STEPS = 18
BATCH = 32
LAT = 4096


def draw_w_qkv(key, part):
    base_key = jax.random.fold_in(key, 0)
    head_size = D // HEADS
    base = jax.random.truncated_normal(base_key, -6.0, 6.0, (D, HEADS, 3, head_size), jnp.float32) / math.sqrt(D)
    return jnp.clip(base, -1.0, 1.0).reshape(D, 3 * D).astype(jnp.bfloat16)


def set_ends(entries, own_key, smallest, high):
    longest = entries.shape.index(max(entries.shape))
    spots = []
    for shift in (0, 1):
        where = [jax.random.randint(jax.random.fold_in(own_key, axis), (), 0, length) for axis, length in enumerate(entries.shape)]
        where[longest] = (where[longest] + shift) % entries.shape[longest]
        spots.append(tuple(where))
    return entries.at[spots[0]].set(smallest).at[spots[1]].set(high)


def block_levels(key, shape, shards, low, top_value):
    factor_of = 1.0
    for dim, blocks in shards:
        steps = jax.random.uniform(jax.random.fold_in(jax.random.fold_in(key, 6), dim), (blocks,), jnp.float32, low / len(shards), top_value / len(shards))
        factor_of = factor_of * jnp.repeat(jnp.exp(steps), shape[dim] // blocks).reshape((-1,) + (1,) * (len(shape) - 1 - dim))
    return factor_of


def gaussian(key, shape, deviation, bound, shards=(), held_as=jnp.bfloat16):
    loudness = block_levels(key, shape, shards, -0.22, 0.18) if shards else 1.0
    entries = jax.random.normal(key, shape, jnp.float32) * deviation * loudness
    return jnp.minimum(jnp.maximum(entries, -bound), bound).astype(held_as)


def setup_inputs(seed: int = 0) -> dict:
    arg_keys = jax.random.split(jax.random.key(seed), 15)
    latents = gaussian(arg_keys[0], (WIN, BATCH, LAT), 1.0, 6.0, ((0, 8), (2, 16)), jnp.float32)
    shifts = set_ends(jax.random.randint(arg_keys[1], (BATCH,), 0, WIN), jax.random.fold_in(arg_keys[1], 1), 0, WIN - 1).astype(jnp.int32)
    starts = set_ends(jax.random.randint(arg_keys[2], (BATCH,), 0, STEPS - 2 * WIN + 1), jax.random.fold_in(arg_keys[2], 1), 0, STEPS - 2 * WIN).astype(jnp.int32)
    labels = set_ends(jax.random.randint(arg_keys[3], (BATCH,), 0, NCLASS), jax.random.fold_in(arg_keys[3], 1), 0, NCLASS - 1).astype(jnp.int32)
    class_table = gaussian(arg_keys[4], (NCLASS, D), 1.0, 6.0)
    w_freq = gaussian(arg_keys[5], (FREQ, D), FREQ ** -0.5, 0.375)
    w_time = gaussian(arg_keys[6], (D, D), D ** -0.5, 0.1875)
    w_ada = gaussian(arg_keys[7], (D, 8 * D), D ** -0.5, 0.1875, ((1, 8),))
    w_patch = gaussian(arg_keys[8], (16, D), 16 ** -0.5, 1.5)
    w_qkv = draw_w_qkv(jax.random.fold_in(arg_keys[14], 71), 0)
    w_proj = gaussian(arg_keys[10], (D, D), D ** -0.5, 0.1875, ((0, 8), (1, 16)))
    w_fc1 = gaussian(arg_keys[11], (D, FF), D ** -0.5, 0.1875, ((0, 16), (1, 8)))
    w_fc2 = gaussian(arg_keys[12], (FF, D), FF ** -0.5, 0.09375, ((0, 8), (1, 16)))
    w_final = gaussian(arg_keys[13], (D, 16), D ** -0.5, 0.1875)
    return dict(latents=latents, shifts=shifts, starts=starts, labels=labels, class_table=class_table, w_freq=w_freq, w_time=w_time, w_ada=w_ada, w_patch=w_patch, w_qkv=w_qkv, w_proj=w_proj, w_fc1=w_fc1, w_fc2=w_fc2, w_final=w_final)


def layer_norm(values):
    average = lax.optimization_barrier(jnp.mean(values, axis=-1, keepdims=True))
    centred = values - average
    variance = lax.optimization_barrier(jnp.mean(centred * centred, axis=-1, keepdims=True))
    return centred * lax.rsqrt(variance + 1e-06)

def position_table(token_count):
    token_ids = jnp.arange(token_count, dtype=jnp.int32)
    row_ids = (token_ids // GRID).astype(jnp.float32)
    col_ids = (token_ids % GRID).astype(jnp.float32)
    quarter = D // 4
    omegas = jnp.exp(-math.log(10000.0) * jnp.arange(quarter, dtype=jnp.float32) / quarter)
    col_angle = col_ids[:, None] * omegas[None, :]
    row_angle = row_ids[:, None] * omegas[None, :]
    return jnp.concatenate([jnp.sin(col_angle), jnp.cos(col_angle), jnp.sin(row_angle), jnp.cos(row_angle)], axis=1)

def cond_activation(step_ids, class_ids, class_table, w_freq, w_time):
    half_freq = FREQ // 2
    freqs = jnp.exp(-math.log(10000.0) * jnp.arange(half_freq, dtype=jnp.float32) / half_freq)
    tvalue = 1000.0 * (1.0 - step_ids.astype(jnp.float32) / STEPS)
    angles = tvalue[:, None] * freqs[None, :]
    embedded = jnp.concatenate([jnp.cos(angles), jnp.sin(angles)], axis=1).astype(jnp.bfloat16)
    hidden_time = jax.nn.silu(jnp.dot(embedded, w_freq, preferred_element_type=jnp.float32)).astype(jnp.bfloat16)
    condition = jnp.dot(hidden_time, w_time, preferred_element_type=jnp.float32) + jnp.take(class_table, class_ids, axis=0).astype(jnp.float32)
    return jax.nn.silu(condition).astype(jnp.bfloat16)

def attend(qkv_rows):
    token_count = qkv_rows.shape[0]
    head_size = D // HEADS
    grouped = qkv_rows.reshape(token_count, HEADS, 3, head_size)
    query = grouped[:, :, 0, :].astype(jnp.float32)
    keys = grouped[:, :, 1, :].astype(jnp.float32)
    values = grouped[:, :, 2, :].astype(jnp.float32)
    scores = jnp.einsum('qhd,khd->hqk', query, keys) * (1.0 / math.sqrt(head_size))
    peak = lax.optimization_barrier(jnp.max(scores, axis=-1, keepdims=True))
    weights = jnp.exp(scores - peak)
    weights = weights / lax.optimization_barrier(jnp.sum(weights, axis=-1, keepdims=True))
    rounded = lax.optimization_barrier(weights.astype(jnp.bfloat16))
    attended = jnp.einsum('hqk,khd->qhd', rounded.astype(jnp.float32), values)
    return attended.astype(jnp.bfloat16).reshape(token_count, HEADS * head_size)

def denoise(point_row, modulation, w_patch, w_qkv, w_proj, w_fc1, w_fc2, w_final):
    patch_size = w_patch.shape[0]
    token_count = point_row.shape[0] // patch_size
    patch_in = point_row.reshape(token_count, patch_size).astype(jnp.bfloat16)
    tokens = jnp.dot(patch_in, w_patch, preferred_element_type=jnp.float32) + position_table(token_count)
    mod_float = modulation.astype(jnp.float32)
    mod_parts = [mod_float[block_index * D:(block_index + 1) * D][None, :] for block_index in range(8)]
    normed = (layer_norm(tokens) * (1.0 + mod_parts[1]) + mod_parts[0]).astype(jnp.bfloat16)
    qkv_rows = jnp.dot(normed, w_qkv, preferred_element_type=jnp.float32).astype(jnp.bfloat16)
    attended = attend(qkv_rows)
    mixed = tokens + mod_parts[2] * jnp.dot(attended, w_proj, preferred_element_type=jnp.float32)
    normed_two = (layer_norm(mixed) * (1.0 + mod_parts[4]) + mod_parts[3]).astype(jnp.bfloat16)
    hidden_units = jax.nn.gelu(jnp.dot(normed_two, w_fc1, preferred_element_type=jnp.float32), approximate=True).astype(jnp.bfloat16)
    residual = mixed + mod_parts[5] * jnp.dot(hidden_units, w_fc2, preferred_element_type=jnp.float32)
    final_in = (layer_norm(residual) * (1.0 + mod_parts[7]) + mod_parts[6]).astype(jnp.bfloat16)
    return jnp.dot(final_in, w_final, preferred_element_type=jnp.float32).astype(jnp.bfloat16).reshape(-1)

def reference(latents, shifts, starts, labels, class_table, w_freq, w_time, w_ada, w_patch, w_qkv, w_proj, w_fc1, w_fc2, w_final):
    positions = jnp.arange(WIN, dtype=jnp.int32)[:, None]
    source_rows = jnp.minimum(positions + shifts[None, :], WIN - 1).astype(jnp.int32)
    points = jnp.take_along_axis(latents, source_rows[:, :, None], axis=0)
    step_ids = (starts + shifts)[None, :] + positions
    class_ids = jnp.broadcast_to(labels[None, :], (WIN, BATCH))
    activation = cond_activation(step_ids.reshape(-1), class_ids.reshape(-1), class_table, w_freq, w_time)
    modulation = jnp.dot(activation, w_ada, preferred_element_type=jnp.float32).astype(jnp.bfloat16)

    def one_point(paired):
        return denoise(paired[0], paired[1], w_patch, w_qkv, w_proj, w_fc1, w_fc2, w_final)
    velocity = lax.map(one_point, (points.reshape(WIN * BATCH, LAT), modulation)).reshape(WIN, BATCH, LAT)
    velocity_float = velocity.astype(jnp.float32)
    summed = jnp.cumsum(velocity_float, axis=0)
    running = jnp.concatenate([jnp.zeros_like(summed[:1]), summed[:-1]], axis=0)
    new_latents = points[0][None] + running * (1.0 / STEPS)
    return (new_latents, velocity)
```

```python
import functools
import math

import jax
import jax.numpy as jnp
from jax import lax
from jax.experimental import pallas as pl
from jax.experimental.pallas import tpu as pltpu
from jax.sharding import PartitionSpec as P

D = 1152
HEADS = 16
FREQ = 256
GRID = 16
STEPS = 18
TOK = 512
BF = jnp.bfloat16
F32 = jnp.float32
MESH_ID = pl.DeviceIdType.MESH

GQ, GP, GF1, GG0, GG3 = 0, 1, 2, 3, 4
GK, GF0, GF2, GG1, GGR = 5, 6, 7, 8, 9
GV, GR, GF3, GG2 = 10, 11, 12, 13
GF = (GF0, GF1, GF2, GF3)
GG = (GG0, GG1, GG2, GG3)
ROUNDS = ((GQ, GK, GV), (GP, GF0, GR), (GF1, GF2, GF3), (GG0, GG1, GG2), (GG3, GGR))
GROUPS = (((0, 2), (5, 2), (10, 2)), ((2, 3), (7, 3), (12, 2)))
NT = (((1,), (1,)), ((), ()))


def part_of(tile):
    return 0 if tile < 5 else (1 if tile < 10 else 2)


def main_kernel(packed, patch, wpatch, mod, wfinal, out, w, xs, nb, att, hid, acc, *sems):
    psend, precv, tsend, trecv, dsend, drecv, lsem = sems
    tm = lax.axis_index("tm")
    ba = lax.axis_index("batch")
    x, c = tm // 2, tm % 2
    z, y = ba // 4, ba % 4
    coord = {"x": x, "y": y, "z": z}

    def device(axis, step):
        at = dict(coord)
        at[axis] = (at[axis] + step + 4) % 4
        return (at["x"] * 2 + c, at["z"] * 4 + at["y"])

    sibling = (x * 2 + 1 - c, ba)

    barrier = pltpu.get_barrier_semaphore()
    for axis in "xyz":
        for step in (1, -1):
            pl.semaphore_signal(barrier, inc=1, device_id=device(axis, step), device_id_type=MESH_ID)
    pl.semaphore_signal(barrier, inc=1, device_id=sibling, device_id_type=MESH_ID)
    pl.semaphore_wait(barrier, 7)

    ORDER = (("y", "z", "x"), ("x", "y", "z"), ("z", "x", "y"))

    def rows(v, start=0, size=72):
        return pl.ds(pl.multiple_of(72 * v + start, 8), size)

    def region(part, phase, g, v, half):
        if phase == 0:
            at = {**coord, ORDER[part][0]: v}
            r = rows(at["y"]) if half is None else (rows(at["y"], 0, 40) if half == 0 else rows(at["y"], 40, 32))
            return w.at[g, at["x"], c, at["z"], r, :]
        two = slice(None) if half is None else pl.ds(2 * half, 2)
        if phase == 1:
            if part == 0:
                return w.at[g, x, c, v, slice(None) if half is None else pl.ds(144 * half, 144), :]
            if part == 1:
                return w.at[g, two, c, z, rows(v), :]
            return w.at[g, v, c, two, rows(y), :]
        if part == 0:
            return w.at[g, v, c, two, :, :]
        if part == 1:
            return w.at[g, two, c, v, :, :]
        return w.at[g, two, c, :, rows(v), :]

    def copies(part, phase, g, send, recv, source=None):
        axis = ORDER[part][phase]
        v = coord[axis]
        up, down = (v + 1) % 4, (v + 3) % 4

        def remote(k):
            if k < 2:
                dst = region(part, phase, g, v, None)
                src = dst if source is None else source
            else:
                src = dst = region(part, phase, g, (down, up)[k - 2], k - 2)
            return pltpu.make_async_remote_copy(
                src_ref=src, dst_ref=dst, send_sem=send(k), recv_sem=recv(k),
                device_id=device(axis, (1, -1)[k % 2]), device_id_type=MESH_ID)

        return [functools.partial(remote, k) for k in range(4)]

    def arrival(part, phase, g, k, send, recv):
        axis = ORDER[part][phase]
        v = coord[axis]
        far = (v + 2) % 4
        ref = (
            region(part, phase, g, (v + 3) % 4, None), region(part, phase, g, (v + 1) % 4, None),
            region(part, phase, g, far, 0), region(part, phase, g, far, 1))[k]
        return pltpu.make_async_copy(ref, ref, recv(k))

    def pre_sems(group, part, phase):
        return (lambda k: psend.at[group, part, phase, k]), (lambda k: precv.at[group, part, phase, k])

    def pre(group, part, phase):
        g0, n = GROUPS[group][part]
        s, r = pre_sems(group, part, phase)
        source = packed.at[pl.ds(g0, n)] if phase == 0 else None
        return copies(part, phase, pl.ds(g0, n), s, r, source)

    def pre_wait(group, part, phase, ks):
        g0, n = GROUPS[group][part]
        s, r = pre_sems(group, part, phase)
        for k in ks:
            arrival(part, phase, pl.ds(g0, n), k, s, r).wait()

    def last(tile):
        return copies(part_of(tile), 2, tile, lambda k: tsend.at[tile, k], lambda k: trecv.at[tile, k])

    def last_wait(tile, ks):
        for k in ks:
            arrival(part_of(tile), 2, tile, k, lambda k: tsend.at[tile, k], lambda k: trecv.at[tile, k]).wait()

    def across(tile):
        return pltpu.make_async_remote_copy(
            src_ref=w.at[tile, :, c], dst_ref=w.at[tile, :, c], send_sem=dsend.at[tile],
            recv_sem=drecv.at[tile], device_id=sibling, device_id_type=MESH_ID)

    def across_wait(tile):
        ref = w.at[tile, :, 1 - c]
        pltpu.make_async_copy(ref, ref, drecv.at[tile]).wait()

    for group in (0, 1):
        for part in range(3):
            for cp in pre(group, part, 0)[:2]:
                cp().start()
    own = pltpu.make_async_copy(packed, w.at[:, x, c, z, rows(y), :], lsem)
    own.start()
    own.wait()
    for phase in (0, 1):
        for group in (0, 1):
            for part in range(3):
                pre_wait(group, part, phase, (0, 1))
                for cp in pre(group, part, phase)[2:]:
                    cp().start()
        for group in (0, 1):
            for part in range(3):
                pre_wait(group, part, phase, (2, 3))
                if phase == 0:
                    for cp in pre(group, part, 1)[:2]:
                        cp().start()
            if phase == 1 and group == 0:
                for r in (0, 1):
                    for tile in ROUNDS[r]:
                        for cp in last(tile)[:2]:
                            cp().start()

    def round_direct(r):
        for tile in ROUNDS[r]:
            last_wait(tile, (0, 1))
            for cp in last(tile)[2:]:
                cp().start()
        if r + 2 < len(ROUNDS):
            for tile in ROUNDS[r + 2]:
                for cp in last(tile)[:2]:
                    cp().start()

    def round_far(r):
        for tile in ROUNDS[r]:
            last_wait(tile, (2, 3))
            across(tile).start()

    def round_ready(r):
        for tile in ROUNDS[r]:
            across_wait(tile)

    def weights(tiles, t):
        return jnp.concatenate([w[g, t // 2, t % 2].reshape(D, 128) for g in tiles], axis=1)

    lane = lax.broadcasted_iota(jnp.int32, (GRID, D), 1)
    quarter = lane // (D // 4)
    omega = jnp.exp(-math.log(10000.0) * (lane - quarter * (D // 4)).astype(F32) / (D // 4))
    angle = lax.broadcasted_iota(jnp.int32, (GRID, D), 0).astype(F32) * omega
    table = jnp.where(quarter % 2 == 0, jnp.sin(angle), jnp.cos(angle))
    acc[0:GRID, :] = table
    lane_low = lane < D // 2
    wp = wpatch[...]

    def tokens_body(i, carry):
        r = i % GRID
        at = pl.ds(pl.multiple_of(i * GRID, GRID), GRID)
        position = jnp.where(lane_low, acc[0:GRID, :], acc[pl.ds(r, 1), :])
        xs[at, :] = jnp.dot(patch[at, :], wp, preferred_element_type=F32) + position
        return carry

    lax.fori_loop(0, TOK // GRID, tokens_body, 0)

    CH = 32

    def norm_rows(load, shift, scale, store):
        def body(i, carry):
            at = pl.ds(pl.multiple_of(i * CH, CH), CH)
            point = i // (TOK // CH // 2)
            v = load(at, point)
            mean = jnp.mean(v, axis=-1, keepdims=True)
            centred = v - mean
            var = jnp.mean(centred * centred, axis=-1, keepdims=True)
            normed = centred * lax.rsqrt(var + 1e-6)
            s = mod[pl.ds(point * 8 + scale, 1), :]
            h = mod[pl.ds(point * 8 + shift, 1), :]
            store(at, (normed * (1.0 + s) + h).astype(BF))
            return carry

        lax.fori_loop(0, TOK // CH, body, 0)

    def store_nb(at, v):
        nb[at, :] = v

    norm_rows(lambda at, point: xs[at, :], 0, 1, store_nb)

    round_direct(0)
    round_far(0)
    round_direct(1)
    round_far(1)
    round_ready(0)
    round_ready(1)

    l256 = lax.broadcasted_iota(jnp.int32, (256, 256), 1)

    def head_lanes(h, rem):
        tile = (l256 >= 64 * h) & (l256 < 64 * h + 64)
        tail = (l256 >= 128 + rem + 8 * h) & (l256 < 128 + rem + 8 * h + 8)
        return tile | tail

    scale = 1.0 / math.sqrt(72.0)

    def attn_body(t, carry):
        wqk = weights((GQ, GK), t)
        wvr = weights((GV, GR), t)

        def one_point(p, carry2):
            at = pl.ds(pl.multiple_of(p * 256, 256), 256)
            xn = nb[at, :]
            qk = jnp.dot(xn, wqk, preferred_element_type=F32)
            vr = jnp.dot(xn, wvr, preferred_element_type=F32)
            rem = vr[:, 128:]
            qq = jnp.concatenate([qk[:, :128], rem], axis=1).astype(BF)
            kk = jnp.concatenate([qk[:, 128:], pltpu.roll(rem, 112, 1)], axis=1).astype(BF)
            vv = jnp.concatenate([vr[:, :128], pltpu.roll(rem, 80, 1)], axis=1).astype(BF)
            outs = []
            for h in (0, 1):
                qh = jnp.where(head_lanes(h, 0), qq, jnp.zeros_like(qq))
                s = lax.dot_general(qh, kk, NT, preferred_element_type=F32)
                m = jnp.max(s, axis=-1, keepdims=True)
                e = jnp.exp((s - m) * scale)
                pb = (e / jnp.sum(e, axis=-1, keepdims=True)).astype(BF)
                outs.append(jnp.dot(pb, vv, preferred_element_type=F32))
            o = jnp.where(head_lanes(0, 112), outs[0], jnp.where(head_lanes(1, 112), outs[1], 0.0))
            att[t, at, :] = o.astype(BF)
            return carry2

        lax.fori_loop(0, 2, one_point, 0)
        return carry

    lax.fori_loop(0, 8, attn_body, 0)

    round_direct(2)
    round_far(2)
    round_ready(2)

    acc[...] = jnp.zeros_like(acc)

    def proj_body(t, carry):
        acc[...] += lax.dot_general(att[t], weights((GP, GR), t), NT, preferred_element_type=F32)
        return carry

    lax.fori_loop(0, 8, proj_body, 0)

    def load_mixed(at, point):
        v = xs[at, :] + mod[pl.ds(point * 8 + 2, 1), :] * acc[at, :]
        xs[at, :] = v
        return v

    norm_rows(load_mixed, 3, 4, store_nb)

    l128 = lax.broadcasted_iota(jnp.int32, (TOK, 128), 1)
    fc1_lanes = (l128 >= 48) & (l128 < 112)

    def fc1_body(t, carry):
        for i in range(2):
            h = jnp.dot(nb[...], weights(GF[2 * i : 2 * i + 2], t), preferred_element_type=F32)
            hid[t, :, 256 * i : 256 * i + 256] = jax.nn.gelu(h, approximate=True).astype(BF)
        h = jnp.dot(nb[...], weights((GR,), t), preferred_element_type=F32)
        hid[t, :, 512:640] = jnp.where(fc1_lanes, jax.nn.gelu(h, approximate=True), 0.0).astype(BF)
        return carry

    lax.fori_loop(0, 8, fc1_body, 0)

    round_direct(3)
    round_far(3)
    round_direct(4)
    round_far(4)
    round_ready(3)
    round_ready(4)

    acc[...] = jnp.zeros_like(acc)

    def fc2_body(t, carry):
        acc[...] += lax.dot_general(
            hid[t], weights((GG0, GG1, GG2, GG3, GGR), t), NT, preferred_element_type=F32)
        return carry

    lax.fori_loop(0, 8, fc2_body, 0)

    def load_residual(at, point):
        return xs[at, :] + mod[pl.ds(point * 8 + 5, 1), :] * acc[at, :]

    norm_rows(load_residual, 6, 7, store_nb)
    out[...] = jnp.dot(nb[...], wfinal[...], preferred_element_type=F32).astype(BF)

    for group in (0, 1):
        for part in range(3):
            for phase in (0, 1):
                for cp in pre(group, part, phase):
                    cp().wait_send()
    for tiles in ROUNDS:
        for tile in tiles:
            for cp in last(tile):
                cp().wait_send()
            across(tile).wait_send()


def denoise(packed, patch, w_patch, mod, w_final):
    vmem = pl.BlockSpec(memory_space=pltpu.VMEM)
    dma = pltpu.SemaphoreType.DMA
    return pl.pallas_call(
        main_kernel,
        out_shape=jax.ShapeDtypeStruct((TOK, 16), BF),
        in_specs=[vmem] * 5,
        out_specs=vmem,
        scratch_shapes=[
            pltpu.VMEM((14, 4, 2, 4, 288, 128), BF),
            pltpu.VMEM((TOK, D), F32),
            pltpu.VMEM((TOK, D), BF),
            pltpu.VMEM((8, TOK, 256), BF),
            pltpu.VMEM((8, TOK, 640), BF),
            pltpu.VMEM((TOK, D), F32),
            dma((2, 3, 2, 4)), dma((2, 3, 2, 4)),
            dma((14, 4)), dma((14, 4)),
            dma((14,)), dma((14,)),
            dma,
        ],
        compiler_params=pltpu.CompilerParams(
            collective_id=0, has_side_effects=True, vmem_limit_bytes=62 * 1024 * 1024),
        name="denoise",
    )(packed, patch, w_patch, mod, w_final)


def pack_weights(w_qkv, w_proj, w_fc1, w_fc2):
    heads = w_qkv.reshape(72, 2, 3, 72)
    main = [heads[:, :, j, :64].reshape(72, 128) for j in range(3)]
    rems = [heads[:, :, j, 64:].reshape(72, 16) for j in range(3)]
    proj = w_proj.T.reshape(72, 2, 72)
    fc2 = w_fc2.T
    tiles = [None] * 14
    tiles[GQ], tiles[GK], tiles[GV] = main
    tiles[GP] = proj[:, :, :64].reshape(72, 128)
    for i in range(4):
        tiles[GF[i]] = w_fc1[:, 128 * i : 128 * i + 128]
        tiles[GG[i]] = fc2[:, 128 * i : 128 * i + 128]
    tiles[GR] = jnp.concatenate(rems + [w_fc1[:, 512:], proj[:, :, 64:].reshape(72, 16)], axis=1)
    tiles[GGR] = jnp.pad(fc2[:, 512:], ((0, 0), (48, 16)))
    return jnp.stack(tiles)


def in_order(parts, dim):
    lengths = list(parts.shape[1:])
    lengths[dim] *= parts.shape[0]
    return jnp.moveaxis(parts, 0, dim).reshape(lengths)


def from_everyone(array, axis):
    copies = jnp.broadcast_to(array, (lax.axis_size(axis), *array.shape))
    return lax.all_to_all(copies, axis, split_axis=0, concat_axis=0, tiled=True)


def gathered_copies(array, axis, dim):
    return in_order(from_everyone(array, axis), dim)


def cond_activation(step_ids, class_ids, class_table, w_freq, w_time):
    half_freq = FREQ // 2
    freqs = jnp.exp(-math.log(10000.0) * jnp.arange(half_freq, dtype=jnp.float32) / half_freq)
    tvalue = 1000.0 * (1.0 - step_ids.astype(jnp.float32) / STEPS)
    angles = tvalue[:, None] * freqs[None, :]
    embedded = jnp.concatenate([jnp.cos(angles), jnp.sin(angles)], axis=1).astype(jnp.bfloat16)
    hidden_time = jax.nn.silu(jnp.dot(embedded, w_freq, preferred_element_type=jnp.float32)).astype(
        jnp.bfloat16
    )
    condition = jnp.dot(hidden_time, w_time, preferred_element_type=jnp.float32) + jnp.take(
        class_table, class_ids, axis=0
    ).astype(jnp.float32)
    return jax.nn.silu(condition).astype(jnp.bfloat16)


def local(
    latents,
    shifts,
    starts,
    labels,
    class_table,
    w_freq,
    w_time,
    w_ada,
    w_patch,
    w_qkv,
    w_proj,
    w_fc1,
    w_fc2,
    w_final,
):
    tm_count = lax.axis_size("tm")
    tm_index = lax.axis_index("tm")
    batch_index = lax.axis_index("batch")
    local_steps = latents.shape[0]
    window = local_steps * tm_count
    whole = gathered_copies(latents, "tm", 0)
    local_positions = tm_index * local_steps + jnp.arange(local_steps, dtype=jnp.int32)[:, None]
    source_rows = jnp.minimum(local_positions + shifts[None, :], window - 1)
    points = jnp.take_along_axis(whole, source_rows[:, :, None], axis=0)
    anchor = jnp.take_along_axis(whole, shifts[None, :, None], axis=0)[0]
    by_sample = lax.all_to_all(
        points.astype(jnp.bfloat16), "batch", split_axis=1, concat_axis=2, tiled=True
    )
    sample_count = by_sample.shape[1]
    lat_count = by_sample.shape[2]
    own_shifts = lax.dynamic_slice_in_dim(shifts, batch_index * sample_count, sample_count)
    own_starts = lax.dynamic_slice_in_dim(starts, batch_index * sample_count, sample_count)
    own_labels = lax.dynamic_slice_in_dim(labels, batch_index * sample_count, sample_count)
    window_positions = jnp.arange(window, dtype=jnp.int32)[:, None]
    step_ids = (own_starts + own_shifts)[None, :] + window_positions
    class_ids = jnp.broadcast_to(own_labels[None, :], step_ids.shape)
    activation = cond_activation(
        step_ids.reshape(-1), class_ids.reshape(-1), class_table, w_freq, w_time
    )
    own_columns = jnp.dot(activation, w_ada, preferred_element_type=jnp.float32).astype(
        jnp.bfloat16
    )
    modulation = lax.all_to_all(own_columns, "tm", split_axis=0, concat_axis=1, tiled=True)
    point_rows = by_sample.reshape(local_steps * sample_count, lat_count)
    point_count = point_rows.shape[0]
    packed = pack_weights(w_qkv, w_proj, w_fc1, w_fc2)
    patch = point_rows.reshape(TOK, 16)
    mod = modulation.astype(F32).reshape(16, D)
    velocity_mid = denoise(packed, patch, w_patch, mod, w_final)
    velocity_mid = velocity_mid.reshape(local_steps, sample_count, lat_count)
    velocity_out = lax.all_to_all(velocity_mid, "batch", split_axis=2, concat_axis=1, tiled=True)
    velocity_float = velocity_out.astype(jnp.float32)
    summed = jnp.cumsum(velocity_float, axis=0)
    running = jnp.concatenate([jnp.zeros_like(summed), summed[:-1]], axis=0)
    block_sum = jnp.sum(velocity_float, axis=0)
    block_sums = gathered_copies(block_sum[None], "tm", 0)
    lower_blocks = jnp.arange(tm_count, dtype=jnp.int32) < tm_index
    earlier_sum = jnp.sum(jnp.where(lower_blocks[:, None, None], block_sums, 0.0), axis=0)
    latents_out = anchor[None] + (earlier_sum[None] + running) * (1.0 / STEPS)
    return (latents_out, velocity_out)


def solution(mesh):
    placed = (
        P("tm", None, "batch"),
        P(),
        P(),
        P(),
        P(),
        P(),
        P(),
        P(None, "tm"),
        P(),
        P("batch", "tm"),
        P("tm", "batch"),
        P("batch", "tm"),
        P("tm", "batch"),
        P(),
    )
    return jax.shard_map(
        local,
        mesh=mesh,
        in_specs=placed,
        out_specs=(P("tm", None, "batch"), P("tm", None, "batch")),
        check_vma=False,
    )
```

```python
import functools
import math

import jax
import jax.numpy as jnp
from jax import lax
from jax.experimental import pallas as pl
from jax.experimental.pallas import tpu as pltpu
from jax.sharding import PartitionSpec as P

D = 1152
HEADS = 16
FREQ = 256
NCLASS = 1001
TM = 8
BA = 16
GRID = 16
STEPS = 18
TOK = 512
BF = jnp.bfloat16
F32 = jnp.float32
MESH_ID = pl.DeviceIdType.MESH

GQ, GP, GF1, GG0, GG3 = 0, 1, 2, 3, 4
GK, GF0, GF2, GG1, GGR = 5, 6, 7, 8, 9
GV, GR, GF3, GG2 = 10, 11, 12, 13
GF = (GF0, GF1, GF2, GF3)
GG = (GG0, GG1, GG2, GG3)
ROUNDS = ((GQ, GK, GV), (GP, GF0, GR), (GF1, GF2, GF3), (GG0, GG1, GG2), (GG3, GGR))
GROUPS = (((0, 2), (5, 2), (10, 2)), ((2, 3), (7, 3), (12, 2)))
NT = (((1,), (1,)), ((), ()))


def part_of(tile):
    return 0 if tile < 5 else (1 if tile < 10 else 2)


def main_kernel(
    shifts, starts, labels, lat, wqkv, wproj, wfc1, wfc2, wpatch, wfinal, ctab, wfreq, wtime, wada,
    lout, vout,
    w, xs, nb, att, hid, acc, packed, win, anchor, ptsend, ptrecv, modsend, modrecv, velsend, velrecv,
    whole, velb, vall, vfreq, vtime, vctab, vada, csem, *sems,
):
    psend, precv, tsend, trecv, dsend, drecv, lsem = sems[:7]
    latsem, ptsem, modsem, velsem, sumsem = [sems[7 + 2 * i : 9 + 2 * i] for i in range(5)]
    tm = lax.axis_index("tm")
    ba = lax.axis_index("batch")
    x, c = tm // 2, tm % 2
    z, y = ba // 4, ba % 4
    coord = {"x": x, "y": y, "z": z}

    def device(axis, step):
        at = dict(coord)
        at[axis] = (at[axis] + step + 4) % 4
        return (at["x"] * 2 + c, at["z"] * 4 + at["y"])

    sibling = (x * 2 + 1 - c, ba)

    barrier = pltpu.get_barrier_semaphore()
    for k in range(1, TM):
        pl.semaphore_signal(barrier, inc=1, device_id=((tm + k) % TM, ba), device_id_type=MESH_ID)
    for k in range(1, BA):
        pl.semaphore_signal(barrier, inc=1, device_id=(tm, (ba + k) % BA), device_id_type=MESH_ID)

    ORDER = (("y", "z", "x"), ("x", "y", "z"), ("z", "x", "y"))

    def rows(v, start=0, size=72):
        return pl.ds(pl.multiple_of(72 * v + start, 8), size)

    def region(part, phase, g, v, half):
        if phase == 0:
            at = {**coord, ORDER[part][0]: v}
            r = rows(at["y"]) if half is None else (rows(at["y"], 0, 40) if half == 0 else rows(at["y"], 40, 32))
            return w.at[g, at["x"], c, at["z"], r, :]
        two = slice(None) if half is None else pl.ds(2 * half, 2)
        if phase == 1:
            if part == 0:
                return w.at[g, x, c, v, slice(None) if half is None else pl.ds(144 * half, 144), :]
            if part == 1:
                return w.at[g, two, c, z, rows(v), :]
            return w.at[g, v, c, two, rows(y), :]
        if part == 0:
            return w.at[g, v, c, two, :, :]
        if part == 1:
            return w.at[g, two, c, v, :, :]
        return w.at[g, two, c, :, rows(v), :]

    def copies(part, phase, g, send, recv, source=None):
        axis = ORDER[part][phase]
        v = coord[axis]
        up, down = (v + 1) % 4, (v + 3) % 4

        def remote(k):
            if k < 2:
                dst = region(part, phase, g, v, None)
                src = dst if source is None else source
            else:
                src = dst = region(part, phase, g, (down, up)[k - 2], k - 2)
            return pltpu.make_async_remote_copy(
                src_ref=src, dst_ref=dst, send_sem=send(k), recv_sem=recv(k),
                device_id=device(axis, (1, -1)[k % 2]), device_id_type=MESH_ID)

        return [functools.partial(remote, k) for k in range(4)]

    def arrival(part, phase, g, k, send, recv):
        axis = ORDER[part][phase]
        v = coord[axis]
        far = (v + 2) % 4
        ref = (
            region(part, phase, g, (v + 3) % 4, None), region(part, phase, g, (v + 1) % 4, None),
            region(part, phase, g, far, 0), region(part, phase, g, far, 1))[k]
        return pltpu.make_async_copy(ref, ref, recv(k))

    def pre_sems(group, part, phase):
        return (lambda k: psend.at[group, part, phase, k]), (lambda k: precv.at[group, part, phase, k])

    def pre(group, part, phase):
        g0, n = GROUPS[group][part]
        s, r = pre_sems(group, part, phase)
        source = packed.at[pl.ds(g0, n)] if phase == 0 else None
        return copies(part, phase, pl.ds(g0, n), s, r, source)

    def pre_wait(group, part, phase, ks):
        g0, n = GROUPS[group][part]
        s, r = pre_sems(group, part, phase)
        for k in ks:
            arrival(part, phase, pl.ds(g0, n), k, s, r).wait()

    def last(tile):
        return copies(part_of(tile), 2, tile, lambda k: tsend.at[tile, k], lambda k: trecv.at[tile, k])

    def last_wait(tile, ks):
        for k in ks:
            arrival(part_of(tile), 2, tile, k, lambda k: tsend.at[tile, k], lambda k: trecv.at[tile, k]).wait()

    def across(tile):
        return pltpu.make_async_remote_copy(
            src_ref=w.at[tile, :, c], dst_ref=w.at[tile, :, c], send_sem=dsend.at[tile],
            recv_sem=drecv.at[tile], device_id=sibling, device_id_type=MESH_ID)

    def across_wait(tile):
        ref = w.at[tile, :, 1 - c]
        pltpu.make_async_copy(ref, ref, drecv.at[tile]).wait()

    def to_tm(k, src, dst, sems):
        return pltpu.make_async_remote_copy(
            src_ref=src, dst_ref=dst, send_sem=sems[0].at[k], recv_sem=sems[1].at[k],
            device_id=((tm + k) % TM, ba), device_id_type=MESH_ID)

    def to_batch(k, src, dst, sems):
        return pltpu.make_async_remote_copy(
            src_ref=src, dst_ref=dst, send_sem=sems[0].at[k], recv_sem=sems[1].at[k],
            device_id=(tm, (ba + k) % BA), device_id_type=MESH_ID)

    def landed(ref, sem):
        pltpu.make_async_copy(ref, ref, sem).wait()

    lat_copy = lambda k: to_tm(k, lat, win.at[tm], latsem)
    pts_copy = lambda k: to_batch(k, ptsend.at[(ba + k) % BA], ptrecv.at[ba], ptsem)
    mod_copy = lambda k: to_tm(k, modsend.at[(tm + k) % TM], modrecv.at[tm], modsem)
    vel_copy = lambda k: to_batch(k, velsend.at[(ba + k) % BA], velrecv.at[ba], velsem)
    sum_copy = lambda k: to_tm(k, velb, vall.at[tm], sumsem)

    conditioning = [
        pltpu.make_async_copy(src, dst, csem.at[i])
        for i, (src, dst) in enumerate(((wfreq, vfreq), (wtime, vtime), (ctab, vctab), (wada, vada)))
    ]
    for cp in conditioning:
        cp.start()

    def lanes_from(count, width, source):
        k = lax.broadcasted_iota(jnp.int32, (count, width), 0)
        n = lax.broadcasted_iota(jnp.int32, (count, width), 1)
        return jnp.where(k == source(n), 1.0, 0.0).astype(BF)

    def qkv_lane(n):
        tile, lane = n // 128, n % 128
        main = 216 * (lane // 64) + 72 * tile + lane % 64
        rem = 216 * ((lane % 16) // 8) + 72 * (lane // 16) + 64 + lane % 8
        return jnp.where(tile < 3, main, jnp.where(lane < 48, rem, -1))

    def proj_lane(n):
        lane = n % 128
        main = 72 * (lane // 64) + lane % 64
        rem = 72 * ((lane - 112) // 8) + 64 + lane % 8
        return jnp.where(n < 128, main, jnp.where(lane >= 112, rem, -1))

    def fc_lane(n):
        return jnp.where((n >= 48) & (n < 112), n - 48, -1)

    q4 = jnp.dot(wqkv[...], lanes_from(432, 512, qkv_lane), preferred_element_type=F32)
    p2 = lax.dot_general(
        wproj[...], lanes_from(144, 256, proj_lane), (((0,), (0,)), ((), ())), preferred_element_type=F32)
    f1 = jnp.dot(wfc1[:, 512:576], lanes_from(64, 128, fc_lane), preferred_element_type=F32)
    f2 = jnp.dot(wfc2[:, 512:576], lanes_from(64, 128, fc_lane), preferred_element_type=F32)
    for i, g in enumerate((GQ, GK, GV)):
        packed[g] = q4[:, 128 * i : 128 * i + 128].astype(BF)
    packed[GR] = (q4[:, 384:] + p2[:, 128:] + f1).astype(BF)
    packed[GP] = p2[:, :128].astype(BF)
    packed[GGR] = f2.astype(BF)
    for i in range(4):
        packed[GF[i]] = wfc1[:, 128 * i : 128 * i + 128]
        packed[GG[i]] = wfc2[:, 128 * i : 128 * i + 128]

    pl.semaphore_wait(barrier, TM + BA - 2)
    for k in range(1, TM):
        lat_copy(k).start()

    for group in (0, 1):
        for part in range(3):
            for cp in pre(group, part, 0)[:2]:
                cp().start()
    own = pltpu.make_async_copy(packed, w.at[:, x, c, z, rows(y), :], lsem)
    own.start()
    own.wait()
    def first_phases(phase):
        for group in (0, 1):
            for part in range(3):
                pre_wait(group, part, phase, (0, 1))
                for cp in pre(group, part, phase)[2:]:
                    cp().start()
        for group in (0, 1):
            for part in range(3):
                pre_wait(group, part, phase, (2, 3))
                if phase == 0:
                    for cp in pre(group, part, 1)[:2]:
                        cp().start()
            if phase == 1 and group == 0:
                for r in (0, 1):
                    for tile in ROUNDS[r]:
                        for cp in last(tile)[:2]:
                            cp().start()

    def round_direct(r):
        for tile in ROUNDS[r]:
            last_wait(tile, (0, 1))
            for cp in last(tile)[2:]:
                cp().start()
        if r + 2 < len(ROUNDS):
            for tile in ROUNDS[r + 2]:
                for cp in last(tile)[:2]:
                    cp().start()

    def round_far(r):
        for tile in ROUNDS[r]:
            last_wait(tile, (2, 3))
            across(tile).start()

    def round_ready(r):
        for tile in ROUNDS[r]:
            across_wait(tile)

    def weights(tiles, t):
        return jnp.concatenate([w[g, t // 2, t % 2].reshape(D, 128) for g in tiles], axis=1)

    CH = 32

    def norm_rows(load, shift, scale, store):
        def body(i, carry):
            at = pl.ds(pl.multiple_of(i * CH, CH), CH)
            point = i // (TOK // CH // 2)
            v = load(at, point)
            mean = jnp.mean(v, axis=-1, keepdims=True)
            centred = v - mean
            var = jnp.mean(centred * centred, axis=-1, keepdims=True)
            normed = centred * lax.rsqrt(var + 1e-6)
            s = modrecv[scale, pl.ds(point, 1), :]
            h = modrecv[shift, pl.ds(point, 1), :]
            store(at, (normed * (1.0 + s) + h).astype(BF))
            return carry

        lax.fori_loop(0, TOK // CH, body, 0)

    def store_nb(at, v):
        nb[at, :] = v

    lane = lax.broadcasted_iota(jnp.int32, (GRID, D), 1)
    quarter = lane // (D // 4)
    omega = jnp.exp(-math.log(10000.0) * (lane - quarter * (D // 4)).astype(F32) / (D // 4))
    angle = lax.broadcasted_iota(jnp.int32, (GRID, D), 0).astype(F32) * omega
    acc[256 : 256 + GRID, :] = jnp.where(quarter % 2 == 0, jnp.sin(angle), jnp.cos(angle))

    def position_body(r, carry):
        at = pl.ds(pl.multiple_of(r * GRID, GRID), GRID)
        acc[at, :] = jnp.where(lane < D // 2, acc[256 : 256 + GRID, :], acc[pl.ds(256 + r, 1), :])
        return carry

    lax.fori_loop(0, GRID, position_body, 0)

    win[tm] = lat[...]
    for k in range(1, TM):
        landed(win.at[(tm + TM - k) % TM], latsem[1].at[k])
    for s in range(32):
        move = shifts[s]
        source = jnp.minimum(tm + move, TM - 1)
        ptsend[s // 2, s % 2 : s % 2 + 1, :] = win[source, s : s + 1, :]
        anchor[s : s + 1, :] = win[move, s : s + 1, :]
    ptrecv[ba] = ptsend[ba]

    first_phases(0)
    for k in range(1, BA):
        pts_copy(k).start()

    row = lax.broadcasted_iota(jnp.int32, (16, 128), 0)
    base = jnp.where(
        row % 2 == 0, starts[2 * ba] + shifts[2 * ba], starts[2 * ba + 1] + shifts[2 * ba + 1])
    tvalue = 1000.0 * (1.0 - (base + row // 2).astype(F32) / STEPS)
    half = FREQ // 2
    freqs = jnp.exp(
        -math.log(10000.0) * lax.broadcasted_iota(jnp.int32, (16, 128), 1).astype(F32) / half)
    angles = tvalue * freqs
    embedded = jnp.concatenate([jnp.cos(angles), jnp.sin(angles)], axis=1).astype(BF)
    for cp in conditioning:
        cp.wait()
    hidden_time = jax.nn.silu(jnp.dot(embedded, vfreq[...], preferred_element_type=F32)).astype(BF)
    which = jnp.where(
        lax.broadcasted_iota(jnp.int32, (16, NCLASS), 0) % 2 == 0, labels[2 * ba], labels[2 * ba + 1])
    one_hot = jnp.where(
        lax.broadcasted_iota(jnp.int32, (16, NCLASS), 1) == which, 1.0, 0.0).astype(BF)
    condition = jnp.dot(hidden_time, vtime[...], preferred_element_type=F32) + jnp.dot(
        one_hot, vctab[...], preferred_element_type=F32)
    activation = jax.nn.silu(condition).astype(BF)
    own_columns = jnp.dot(activation, vada[...], preferred_element_type=F32).astype(BF).astype(F32)
    for j in range(TM):
        modsend[j] = own_columns[2 * j : 2 * j + 2, :]
    modrecv[tm] = modsend[tm]

    for k in range(1, BA):
        landed(ptrecv.at[(ba + BA - k) % BA], ptsem[1].at[k])
    for k in range(1, TM):
        mod_copy(k).start()
    own_patch = lax.broadcasted_iota(jnp.int32, (GRID, 256), 1) // 16 == lax.broadcasted_iota(
        jnp.int32, (GRID, 256), 0)
    for p in range(2):
        for b in range(BA):
            values = jnp.where(own_patch, ptrecv[b, p : p + 1, :], 0.0)
            att[0, 256 * p + 16 * b : 256 * p + 16 * b + 16, :] = values.astype(BF)
    wp = jnp.concatenate([wpatch[...]] * 16, axis=0)
    for i in range(4):
        at = slice(128 * i, 128 * i + 128)
        position = acc[128 * (i % 2) : 128 * (i % 2) + 128, :]
        xs[at, :] = jnp.dot(att[0, at, :], wp, preferred_element_type=F32) + position

    first_phases(1)
    for k in range(1, TM):
        landed(modrecv.at[(tm + TM - k) % TM], modsem[1].at[k])
    norm_rows(lambda at, point: xs[at, :], 0, 1, store_nb)

    round_direct(0)
    round_far(0)
    round_direct(1)
    round_far(1)
    round_ready(0)
    round_ready(1)

    l256 = lax.broadcasted_iota(jnp.int32, (256, 256), 1)

    def head_lanes(h, rem):
        tile = (l256 >= 64 * h) & (l256 < 64 * h + 64)
        tail = (l256 >= 128 + rem + 8 * h) & (l256 < 128 + rem + 8 * h + 8)
        return tile | tail

    scale = 1.0 / math.sqrt(72.0)

    def attn_body(t, carry):
        wqk = weights((GQ, GK), t)
        wvr = weights((GV, GR), t)

        def one_point(p, carry2):
            at = pl.ds(pl.multiple_of(p * 256, 256), 256)
            xn = nb[at, :]
            qk = jnp.dot(xn, wqk, preferred_element_type=F32)
            vr = jnp.dot(xn, wvr, preferred_element_type=F32)
            rem = vr[:, 128:]
            qq = jnp.concatenate([qk[:, :128], rem], axis=1).astype(BF)
            kk = jnp.concatenate([qk[:, 128:], pltpu.roll(rem, 112, 1)], axis=1).astype(BF)
            vv = jnp.concatenate([vr[:, :128], pltpu.roll(rem, 80, 1)], axis=1).astype(BF)
            outs = []
            for h in (0, 1):
                qh = jnp.where(head_lanes(h, 0), qq, jnp.zeros_like(qq))
                s = lax.dot_general(qh, kk, NT, preferred_element_type=F32)
                m = jnp.max(s, axis=-1, keepdims=True)
                e = jnp.exp((s - m) * scale)
                pb = (e / jnp.sum(e, axis=-1, keepdims=True)).astype(BF)
                outs.append(jnp.dot(pb, vv, preferred_element_type=F32))
            o = jnp.where(head_lanes(0, 112), outs[0], jnp.where(head_lanes(1, 112), outs[1], 0.0))
            att[t, at, :] = o.astype(BF)
            return carry2

        lax.fori_loop(0, 2, one_point, 0)
        return carry

    lax.fori_loop(0, 8, attn_body, 0)

    round_direct(2)
    round_far(2)
    round_ready(2)

    acc[...] = jnp.zeros_like(acc)

    def proj_body(t, carry):
        acc[...] += lax.dot_general(att[t], weights((GP, GR), t), NT, preferred_element_type=F32)
        return carry

    lax.fori_loop(0, 8, proj_body, 0)

    def load_mixed(at, point):
        v = xs[at, :] + modrecv[2, pl.ds(point, 1), :] * acc[at, :]
        xs[at, :] = v
        return v

    norm_rows(load_mixed, 3, 4, store_nb)

    l128 = lax.broadcasted_iota(jnp.int32, (TOK, 128), 1)
    fc1_lanes = (l128 >= 48) & (l128 < 112)

    def fc1_body(t, carry):
        for i in range(2):
            h = jnp.dot(nb[...], weights(GF[2 * i : 2 * i + 2], t), preferred_element_type=F32)
            hid[t, :, 256 * i : 256 * i + 256] = jax.nn.gelu(h, approximate=True).astype(BF)
        h = jnp.dot(nb[...], weights((GR,), t), preferred_element_type=F32)
        hid[t, :, 512:640] = jnp.where(fc1_lanes, jax.nn.gelu(h, approximate=True), 0.0).astype(BF)
        return carry

    lax.fori_loop(0, 8, fc1_body, 0)

    round_direct(3)
    round_far(3)
    round_direct(4)
    round_far(4)
    round_ready(3)
    round_ready(4)

    acc[...] = jnp.zeros_like(acc)

    def fc2_body(t, carry):
        acc[...] += lax.dot_general(
            hid[t], weights((GG0, GG1, GG2, GG3, GGR), t), NT, preferred_element_type=F32)
        return carry

    lax.fori_loop(0, 8, fc2_body, 0)

    def load_residual(at, point):
        return xs[at, :] + modrecv[5, pl.ds(point, 1), :] * acc[at, :]

    norm_rows(load_residual, 6, 7, store_nb)
    wf = jnp.concatenate([wfinal[...]] * 16, axis=0)
    v = lax.dot_general(nb[...], wf, NT, preferred_element_type=F32)
    own_value = lax.broadcasted_iota(jnp.int32, (TOK, 256), 1) // 16 == lax.broadcasted_iota(
        jnp.int32, (TOK, 256), 0) % 16
    v = jnp.where(own_value, v, 0.0).astype(BF)
    out_row = lax.broadcasted_iota(jnp.int32, (32, TOK), 0)
    token = lax.broadcasted_iota(jnp.int32, (32, TOK), 1)
    pick = (out_row % 2 == token // 256) & (out_row // 2 == (token % 256) // 16)
    v = jnp.dot(jnp.where(pick, 1.0, 0.0).astype(BF), v, preferred_element_type=F32)
    for b in range(BA):
        velsend[b] = v[2 * b : 2 * b + 2, :]
    velrecv[ba] = velsend[ba]

    for group in (0, 1):
        for part in range(3):
            for phase in (0, 1):
                for cp in pre(group, part, phase):
                    cp().wait_send()
    for tiles in ROUNDS:
        for tile in tiles:
            for cp in last(tile):
                cp().wait_send()
            across(tile).wait_send()
    for k in range(1, TM):
        lat_copy(k).wait_send()
        mod_copy(k).wait_send()
    for k in range(1, BA):
        pts_copy(k).wait_send()

    for k in range(1, BA):
        vel_copy(k).start()
    for k in range(1, BA):
        landed(velrecv.at[(ba + BA - k) % BA], velsem[1].at[k])
    for b in range(BA):
        whole[2 * b : 2 * b + 2, :] = velrecv[b]
    velocity = whole[...]
    velb[...] = velocity.astype(BF)
    vout[0] = velocity.astype(BF)
    vall[tm] = velocity.astype(BF)
    for k in range(1, BA):
        vel_copy(k).wait_send()

    for k in range(1, TM):
        sum_copy(k).start()
    for k in range(1, TM):
        landed(vall.at[(tm + TM - k) % TM], sumsem[1].at[k])
    total = jnp.zeros((32, 256), F32)
    for i in range(TM):
        total = total + jnp.where(i < tm, vall[i].astype(F32), 0.0)
    lout[0] = anchor[...] + total * (1.0 / STEPS)
    for k in range(1, TM):
        sum_copy(k).wait_send()


def local(latents, shifts, starts, labels, class_table, w_freq, w_time, w_ada, w_patch, w_qkv, w_proj,
          w_fc1, w_fc2, w_final):
    vmem = pl.BlockSpec(memory_space=pltpu.VMEM)
    smem = pl.BlockSpec(memory_space=pltpu.SMEM)
    hbm = pl.BlockSpec(memory_space=pl.ANY)
    dma = pltpu.SemaphoreType.DMA
    vm = pltpu.VMEM
    return pl.pallas_call(
        main_kernel,
        out_shape=(
            jax.ShapeDtypeStruct((1, 32, 256), F32),
            jax.ShapeDtypeStruct((1, 32, 256), BF),
        ),
        in_specs=[smem] * 3 + [vmem] * 7 + [hbm] * 4,
        out_specs=(vmem, vmem),
        scratch_shapes=[
            vm((14, 4, 2, 4, 288, 128), BF),
            vm((TOK, D), F32),
            vm((TOK, D), BF),
            vm((8, TOK, 256), BF),
            vm((8, TOK, 640), BF),
            vm((TOK, D), F32),
            vm((14, 72, 128), BF),
            vm((TM, 32, 256), F32),
            vm((32, 256), F32),
            vm((BA, 2, 256), F32), vm((BA, 2, 256), F32),
            vm((TM, 2, D), F32), vm((TM, 2, D), F32),
            vm((BA, 2, 256), F32), vm((BA, 2, 256), F32),
            vm((32, 256), F32),
            vm((32, 256), BF),
            vm((TM, 32, 256), BF),
            vm((FREQ, D), BF), vm((D, D), BF), vm((NCLASS, D), BF), vm((D, D), BF),
            dma((4,)),
            dma((2, 3, 2, 4)), dma((2, 3, 2, 4)),
            dma((14, 4)), dma((14, 4)),
            dma((14,)), dma((14,)),
            dma,
            dma((TM,)), dma((TM,)),
            dma((BA,)), dma((BA,)),
            dma((TM,)), dma((TM,)),
            dma((BA,)), dma((BA,)),
            dma((TM,)), dma((TM,)),
        ],
        compiler_params=pltpu.CompilerParams(
            collective_id=0, has_side_effects=True, vmem_limit_bytes=63 * 1024 * 1024),
        name="denoise",
    )(shifts, starts, labels, latents.reshape(32, 256), w_qkv, w_proj, w_fc1, w_fc2.T, w_patch,
      w_final.T, class_table, w_freq, w_time, w_ada)


def solution(mesh):
    placed = (
        P("tm", None, "batch"),
        P(),
        P(),
        P(),
        P(),
        P(),
        P(),
        P(None, "tm"),
        P(),
        P("batch", "tm"),
        P("tm", "batch"),
        P("batch", "tm"),
        P("tm", "batch"),
        P(),
    )
    return jax.shard_map(
        local,
        mesh=mesh,
        in_specs=placed,
        out_specs=(P("tm", None, "batch"), P("tm", None, "batch")),
        check_vma=False,
    )
```
